32 devices in a mesh: dp: 2 (over x), tp: 4 (over z), fsdp: 4 (over y, core).
Axes of the slice: x: 2, y: 2, z: 4, core: 2. Of those that a mesh axis runs over, the one named last changes fastest.
Arguments:
- x_in: bfloat16 [8, 2048, 3072], P(('dp', 'fsdp')), parts along dimension 0
- seq_lens: int32 [8], P(('dp', 'fsdp')), parts along dimension 0
- ln1_gain: bfloat16 [3072], replicated
- w_q: bfloat16 [3072, 32, 128], P('fsdp', 'tp')
- w_k: bfloat16 [3072, 8, 128], P('fsdp', 'tp')
- w_v: bfloat16 [3072, 8, 128], P('fsdp', 'tp')
- w_o: bfloat16 [32, 128, 3072], P('tp', None, 'fsdp')
- ln2_gain: bfloat16 [3072], replicated
- w_up: bfloat16 [3072, 9216], P('fsdp', 'tp')
- w_down: bfloat16 [9216, 3072], P('tp', 'fsdp')
Outputs:
- output 1: bfloat16 [8, 2048, 3072], P(('dp', 'fsdp')), parts along dimension 0
- output 2: bfloat16 [8, 2048, 8, 128], P(('dp', 'fsdp'), None, 'tp'), parts along dimension 0
- output 3: bfloat16 [8, 2048, 8, 128], P(('dp', 'fsdp'), None, 'tp'), parts along dimension 0
There are 2 independent parts. The reference program is written for one: setup_inputs(seed, part) draws one part's arguments, and reference() takes and returns one part's arrays. A program takes and returns all parts, laid end to end along the dimension named above; an argument that names none is the same for every part.
All inputs are finite; a program needn't handle non-finite values.
Results may differ from the reference program's by a relative error of at most 0.02.
Values are sent between devices in bfloat16 or wider.
A program may use at most 1 GiB of HBM per device.

```python
import jax
import jax.numpy as jnp
from jax import lax

BATCH = 4
SEQ = 2048
D = 3072
HEADS = 32
KV_HEADS = 8
HEAD = 128
FF = 9216
ROT = HEAD // 2
EPS = 1e-5
ROPE_BASE = 10000.0


def setup_inputs(seed: int = 0, part: int = 0) -> dict:
    base_key = jax.random.key(seed)
    part_key = jax.random.fold_in(base_key, part)
    w_keys = jax.random.split(base_key, 8)
    x_in = jax.random.normal(jax.random.fold_in(part_key, 0), (BATCH, SEQ, D), jnp.float32).astype(jnp.bfloat16)
    seq_lens = jax.random.randint(jax.random.fold_in(part_key, 1), (BATCH,), SEQ // 8, SEQ + 1, dtype=jnp.int32)
    seq_lens = seq_lens.at[0].set(SEQ).at[1].set(SEQ // 8)
    ln1_gain = (0.5 * jax.random.normal(w_keys[0], (D,), jnp.float32)).astype(jnp.bfloat16)
    w_q = (jax.random.normal(w_keys[1], (D, HEADS, HEAD), jnp.float32) * D ** -0.5).astype(jnp.bfloat16)
    w_k = (jax.random.normal(w_keys[2], (D, KV_HEADS, HEAD), jnp.float32) * D ** -0.5).astype(jnp.bfloat16)
    w_v = (jax.random.normal(w_keys[3], (D, KV_HEADS, HEAD), jnp.float32) * D ** -0.5).astype(jnp.bfloat16)
    w_o = (jax.random.normal(w_keys[4], (HEADS, HEAD, D), jnp.float32) * (HEADS * HEAD) ** -0.5 * SEQ ** 0.25).astype(jnp.bfloat16)
    ln2_gain = (0.5 * jax.random.normal(w_keys[5], (D,), jnp.float32)).astype(jnp.bfloat16)
    w_up = (jax.random.normal(w_keys[6], (D, FF), jnp.float32) * D ** -0.5).astype(jnp.bfloat16)
    w_down = (jax.random.normal(w_keys[7], (FF, D), jnp.float32) * FF ** -0.5).astype(jnp.bfloat16)
    return {"x_in": x_in, "seq_lens": seq_lens, "ln1_gain": ln1_gain, "w_q": w_q, "w_k": w_k, "w_v": w_v, "w_o": w_o, "ln2_gain": ln2_gain, "w_up": w_up, "w_down": w_down}


def layer_norm(x_rows, gain_vec):
    x_f32 = x_rows.astype(jnp.float32)
    mean_x = jnp.mean(x_f32, axis=-1, keepdims=True)
    centred = x_f32 - mean_x
    var_x = jnp.mean(centred * centred, axis=-1, keepdims=True)
    return (centred * lax.rsqrt(var_x + EPS) * (1.0 + gain_vec.astype(jnp.float32))).astype(jnp.bfloat16)


def rotary(t_heads):
    half_rot = ROT // 2
    inv_freq = ROPE_BASE ** (-2.0 * jnp.arange(half_rot, dtype=jnp.float32) / ROT)
    angles = jnp.arange(SEQ, dtype=jnp.float32)[:, None] * inv_freq[None, :]
    cos_t = jnp.cos(angles)[:, None, :]
    sin_t = jnp.sin(angles)[:, None, :]
    t_f32 = t_heads.astype(jnp.float32)
    first_half = t_f32[..., :half_rot]
    second_half = t_f32[..., half_rot:ROT]
    return jnp.concatenate([first_half * cos_t - second_half * sin_t, second_half * cos_t + first_half * sin_t, t_f32[..., ROT:]], axis=-1).astype(jnp.bfloat16)


def reference(x_in, seq_lens, ln1_gain, w_q, w_k, w_v, w_o, ln2_gain, w_up, w_down):
    q_per_kv = HEADS // KV_HEADS
    w_q2 = w_q.reshape(D, HEADS * HEAD)
    w_k2 = w_k.reshape(D, KV_HEADS * HEAD)
    w_v2 = w_v.reshape(D, KV_HEADS * HEAD)
    w_o2 = w_o.reshape(HEADS * HEAD, D)
    positions = jnp.arange(SEQ)
    causal = positions[None, :] <= positions[:, None]

    def one_sequence(seq_pair):
        x_row, seq_len = seq_pair
        h_norm = layer_norm(x_row, ln1_gain)
        q_all = jnp.dot(h_norm, w_q2, preferred_element_type=jnp.float32).astype(jnp.bfloat16).reshape(SEQ, HEADS, HEAD)
        k_all = jnp.dot(h_norm, w_k2, preferred_element_type=jnp.float32).astype(jnp.bfloat16).reshape(SEQ, KV_HEADS, HEAD)
        v_all = jnp.dot(h_norm, w_v2, preferred_element_type=jnp.float32).astype(jnp.bfloat16).reshape(SEQ, KV_HEADS, HEAD)
        q_rot = rotary(q_all)
        k_rot = rotary(k_all)
        allowed = causal & (positions[None, :] < seq_len)
        q_groups = jnp.swapaxes(q_rot.reshape(SEQ, KV_HEADS, q_per_kv, HEAD), 0, 1)

        def one_kv_head(head_trio):
            q_head, k_head, v_head = head_trio
            scores = jnp.einsum("qgd,sd->gqs", q_head.astype(jnp.float32), k_head.astype(jnp.float32)) * HEAD ** -0.5
            attn_probs = jax.nn.softmax(jnp.where(allowed[None], scores, -1e30), axis=-1).astype(jnp.bfloat16)
            return jnp.einsum("gqs,sd->qgd", attn_probs.astype(jnp.float32), v_head.astype(jnp.float32)).astype(jnp.bfloat16)

        context = lax.map(one_kv_head, (q_groups, jnp.swapaxes(k_rot, 0, 1), jnp.swapaxes(v_all, 0, 1)))
        context = jnp.swapaxes(context, 0, 1).reshape(SEQ, HEADS * HEAD)
        attn_out = jnp.dot(context, w_o2, preferred_element_type=jnp.float32)
        x_mid = (x_row.astype(jnp.float32) + attn_out).astype(jnp.bfloat16)
        h_mid = layer_norm(x_mid, ln2_gain)
        up_act = jnp.dot(h_mid, w_up, preferred_element_type=jnp.float32)
        relu_sq = jnp.square(jnp.maximum(up_act, 0.0)).astype(jnp.bfloat16)
        down_out = jnp.dot(relu_sq, w_down, preferred_element_type=jnp.float32)
        y_row = (x_mid.astype(jnp.float32) + down_out).astype(jnp.bfloat16)
        return y_row, k_rot, v_all

    y_rows, k_rows, v_rows = lax.map(one_sequence, (x_in, seq_lens))
    return y_rows, k_rows, v_rows
```

```python
import functools

import jax
import jax.numpy as jnp
from jax import lax
from jax.experimental import pallas as pl
from jax.experimental.pallas import tpu as pltpu
from jax.sharding import PartitionSpec as P

EPS = 1e-5
ROPE_BASE = 10000.0
PIECES = 8
LAG = 2
QBLK = 256
KBLK = 512


def layer_norm(x_rows, gain_vec):
    x_f32 = x_rows.astype(jnp.float32)
    mean_x = jnp.mean(x_f32, axis=-1, keepdims=True)
    centred = x_f32 - mean_x
    var_x = jnp.mean(centred * centred, axis=-1, keepdims=True)
    return (centred * lax.rsqrt(var_x + EPS) * (1.0 + gain_vec.astype(jnp.float32))).astype(jnp.bfloat16)


def rotary_tables(seq_length, head_dim):
    rot_dims = head_dim // 2
    half_rot = rot_dims // 2
    inv_freq = ROPE_BASE ** (-2.0 * jnp.arange(half_rot, dtype=jnp.float32) / rot_dims)
    angles = jnp.arange(seq_length, dtype=jnp.float32)[:, None] * inv_freq[None, :]
    cos_t, sin_t = jnp.cos(angles), jnp.sin(angles)
    zeros = jnp.zeros_like(sin_t)
    tail = jnp.zeros((seq_length, head_dim - rot_dims), jnp.float32)
    keep = jnp.concatenate([cos_t, cos_t, tail + 1.0], axis=1)
    from_low = jnp.concatenate([zeros, sin_t, tail], axis=1)
    from_high = jnp.concatenate([-sin_t, zeros, tail], axis=1)
    return keep, from_low, from_high


def rotate(t_bf16, keep, from_low, from_high):
    head_dim = t_bf16.shape[1]
    quarter = head_dim // 4
    t_f32 = t_bf16.astype(jnp.float32)
    low = pltpu.roll(t_f32, quarter, 1)
    high = pltpu.roll(t_f32, head_dim - quarter, 1)
    return (t_f32 * keep + low * from_low + high * from_high).astype(jnp.bfloat16)


def attention_kernel(first, group_id, len_ref, q_ref, k_ref, v_ref, qc_ref, ql_ref, qh_ref, *rest):
    if first:
        kc_ref, kl_ref, kh_ref, ctx_ref, k_rot_ref = rest
    else:
        ctx_ref, k_rot_ref = rest[0], k_ref
    strip = pl.program_id(1)
    head_dim = k_ref.shape[1]
    heads = q_ref.shape[1] // head_dim
    half = k_ref.shape[0] // 2

    if first:

        @pl.when(strip == 0)
        def _():
            k_rot_ref[...] = rotate(k_ref[...], kc_ref[...], kl_ref[...], kh_ref[...])

    seq_len = len_ref[0]
    scale = head_dim ** -0.5
    row0 = strip * half + group_id * QBLK
    n_keys = jnp.minimum(row0 + QBLK, seq_len)
    n_blocks = (n_keys + KBLK - 1) // KBLK
    n_clear = jnp.minimum(row0, seq_len) // KBLK
    tables = (qc_ref[...], ql_ref[...], qh_ref[...])
    q_rot = [rotate(q_ref[:, h * head_dim:(h + 1) * head_dim], *tables) for h in range(heads)]

    def step(masked, kb, carry):
        start = pl.multiple_of(kb * KBLK, KBLK)
        k_blk = k_rot_ref[pl.ds(start, KBLK), :]
        v_blk = v_ref[pl.ds(start, KBLK), :]
        if masked:
            rows = row0 + lax.broadcasted_iota(jnp.int32, (QBLK, KBLK), 0)
            cols = start + lax.broadcasted_iota(jnp.int32, (QBLK, KBLK), 1)
            allowed = (cols <= rows) & (cols < seq_len)
        out = []
        for h in range(heads):
            m_old, l_old, acc = carry[h]
            s = lax.dot_general(q_rot[h], k_blk, (((1,), (1,)), ((), ())), preferred_element_type=jnp.float32) * scale
            if masked:
                s = jnp.where(allowed, s, -1e30)
            m_new = jnp.maximum(m_old, jnp.max(s, axis=1, keepdims=True))
            corr = jnp.exp(m_old - m_new)
            p = jnp.exp(s - m_new)
            l_new = l_old * corr + jnp.sum(p, axis=1, keepdims=True)
            acc = acc * corr + jnp.dot(p.astype(jnp.bfloat16), v_blk, preferred_element_type=jnp.float32)
            out.append((m_new, l_new, acc))
        return tuple(out)

    init = tuple(
        (jnp.full((QBLK, 1), -1e30, jnp.float32), jnp.zeros((QBLK, 1), jnp.float32), jnp.zeros((QBLK, head_dim), jnp.float32))
        for _ in range(heads)
    )
    carry = lax.fori_loop(0, n_clear, functools.partial(step, False), init)
    carry = lax.fori_loop(n_clear, n_blocks, functools.partial(step, True), carry)
    for h in range(heads):
        _, l_sum, acc = carry[h]
        ctx_ref[:, h * head_dim:(h + 1) * head_dim] = (acc / l_sum).astype(jnp.bfloat16)


def attend(group_id, qkv, k_rot, seq_lens, tables, q_heads, kv_heads, head_dim):
    first = k_rot is None
    seq_length = qkv.shape[0]
    width = q_heads // kv_heads * head_dim
    strips = seq_length // 2 // QBLK
    q_spec = pl.BlockSpec((QBLK, width), lambda g, i, *_: (i * strips + group_id, g))
    table_q = pl.BlockSpec((QBLK, head_dim), lambda g, i, *_: (i * strips + group_id, 0))
    table_k = pl.BlockSpec((seq_length, head_dim), lambda g, i, *_: (0, 0))
    k_base = q_heads if first else 0
    k_spec = pl.BlockSpec((seq_length, head_dim), lambda g, i, *_: (0, k_base + g))
    v_spec = pl.BlockSpec((seq_length, head_dim), lambda g, i, *_: (0, q_heads + kv_heads + g))
    out_specs = [pl.BlockSpec((QBLK, width), lambda g, i, *_: (i, g))]
    out_shape = [jax.ShapeDtypeStruct((2 * QBLK, q_heads * head_dim), jnp.bfloat16)]
    if first:
        out_specs.append(pl.BlockSpec((seq_length, head_dim), lambda g, i, *_: (0, g)))
        out_shape.append(jax.ShapeDtypeStruct((seq_length, kv_heads * head_dim), jnp.bfloat16))
    keys = seq_length // 2 + (2 * group_id + 1) * QBLK
    return pl.pallas_call(
        functools.partial(attention_kernel, first, group_id),
        grid_spec=pltpu.PrefetchScalarGridSpec(
            num_scalar_prefetch=1,
            grid=(kv_heads, 2),
            in_specs=[q_spec, k_spec, v_spec] + [table_q] * 3 + ([table_k] * 3 if first else []),
            out_specs=out_specs,
        ),
        out_shape=out_shape,
        compiler_params=pltpu.CompilerParams(dimension_semantics=("arbitrary", "arbitrary"), vmem_limit_bytes=48 << 20),
        cost_estimate=pl.CostEstimate(flops=12 * q_heads * head_dim * QBLK * keys, bytes_accessed=4 << 20, transcendentals=q_heads * QBLK * keys),
        name="attend",
    )(seq_lens, qkv, qkv if first else k_rot, qkv, *tables, *(tables if first else ()))


def solution(mesh):
    batch_axes = ("dp", "fsdp")
    arg_specs = (P(batch_axes, None, None), P(batch_axes), P(None), P("fsdp", "tp", None), P("fsdp", "tp", None), P("fsdp", "tp", None), P("tp", None, "fsdp"), P(None), P("fsdp", "tp"), P("tp", "fsdp"))
    out_parts = (P(batch_axes, None, None), P(batch_axes, None, "tp", None), P(batch_axes, None, "tp", None))
    n_tp = mesh.shape["tp"]
    last = n_tp - 1
    rightward = [(k, k + 1) for k in range(last)]
    leftward = [(k + 1, k) for k in range(last)]

    def layer_local(x_in, seq_lens, ln1_gain, w_q, w_k, w_v, w_o, ln2_gain, w_up, w_down):
        _, seq_length, width = x_in.shape
        q_heads, kv_heads, head_dim = w_q.shape[1], w_k.shape[1], w_k.shape[2]
        half = seq_length // 2
        rows = half // PIECES
        z = lax.axis_index("tp")
        x_rows = x_in.reshape(seq_length, width)

        w_qkv = jnp.concatenate([w.reshape(w.shape[0], -1) for w in (w_q, w_k, w_v)], axis=1)
        qkv_full = lax.all_gather(w_qkv, "fsdp", axis=0, tiled=True)
        o_full = lax.all_gather(w_o.reshape(q_heads * head_dim, -1), "fsdp", axis=1, tiled=True)
        up_full = lax.all_gather(w_up, "fsdp", axis=0, tiled=True)
        down_full = lax.all_gather(w_down, "fsdp", axis=1, tiled=True)

        tables = rotary_tables(seq_length, head_dim)
        h_norm = layer_norm(x_rows, ln1_gain)
        qkv = jnp.dot(h_norm, qkv_full, preferred_element_type=jnp.float32).astype(jnp.bfloat16)
        n_groups = half // QBLK
        per_group = QBLK // rows
        k_rot = None
        o_parts, mlp_parts = [], []
        for g in range(n_groups):
            ctx, *rotated = attend(g, qkv, k_rot, seq_lens, tables, q_heads, kv_heads, head_dim)
            k_rot = rotated[0] if rotated else k_rot
            o_parts.append(jnp.dot(ctx, o_full, preferred_element_type=jnp.float32).astype(jnp.bfloat16))
        v_loc = qkv[:, (q_heads + kv_heads) * head_dim:]

        place = (z, last - z)
        base = (half, 0)
        own_row = jnp.where(z == last, half, 0)
        steps = 4 * PIECES + last * LAG
        received, sent = {}, {}
        h_own, x_own, y_own = {}, {}, {}
        out = jnp.zeros((seq_length, width), jnp.bfloat16)

        def by_place(d, options):
            value = None
            for j, option in options:
                value = option if value is None else jnp.where(place[d] == j, option, value)
            return value

        def partial_sum(parts, order, d):
            options = []
            for j in range(n_tp):
                p = order - LAG * j
                if 0 <= p < PIECES:
                    row = (1 - d) * QBLK + (p % per_group) * rows
                    options.append((j, parts[p // per_group][row:row + rows]))
            return by_place(d, options)

        def mlp_group(g):
            pieces = []
            for d in range(2):
                for p in range(g * per_group, (g + 1) * per_group):
                    pieces.append(by_place(d, [(j, sent[(PIECES + p + LAG * j, d)]) for j in range(n_tp)]))
            h_rows = jnp.concatenate(pieces, axis=0)
            up_act = jnp.dot(h_rows, up_full, preferred_element_type=jnp.float32)
            relu_sq = jnp.square(jnp.maximum(up_act, 0.0)).astype(jnp.bfloat16)
            return jnp.dot(relu_sq, down_full, preferred_element_type=jnp.float32).astype(jnp.bfloat16)

        for t in range(steps):
            phases = sorted({(t - LAG * j) // PIECES for j in range(n_tp) if 0 <= t - LAG * j < 4 * PIECES})
            if 2 in phases and len(mlp_parts) <= min(t - 2 * PIECES, PIECES - 1) // per_group:
                mlp_parts.append(mlp_group(len(mlp_parts)))
            for d, hops in enumerate((rightward, leftward)):
                got = received.get((t - LAG, d))
                for phase in phases:
                    if phase in (0, 2):
                        value = partial_sum((o_parts, mlp_parts)[phase // 2], t - phase * PIECES, d)
                        if got is not None:
                            value = (value.astype(jnp.float32) + got.astype(jnp.float32)).astype(jnp.bfloat16)
                    else:
                        own = (h_own, y_own)[phase // 2][min(t - phase * PIECES, PIECES - 1)]
                        value = jnp.where(place[d] == 0, own, got)
                    if (t, d) in sent:
                        value = jnp.where(t - LAG * place[d] >= phase * PIECES, value, sent[(t, d)])
                    sent[(t, d)] = value
                if t < steps - LAG:
                    received[(t, d)] = lax.ppermute(sent[(t, d)], "tp", hops)
            done = t - last * LAG
            if 0 <= done < PIECES or 2 * PIECES <= done < 3 * PIECES:
                total = jnp.where(z == last, sent[(t, 0)], sent[(t, 1)]).astype(jnp.float32)
                p = done % PIECES
                if done < PIECES:
                    x_piece = lax.dynamic_slice_in_dim(x_rows, own_row + p * rows, rows, axis=0).astype(jnp.float32)
                    x_own[p] = (x_piece + total).astype(jnp.bfloat16)
                    h_own[p] = layer_norm(x_own[p], ln2_gain)
                else:
                    y_own[p] = (x_own[p].astype(jnp.float32) + total).astype(jnp.bfloat16)
            if 3 in phases:
                for d in range(2):
                    p = jnp.clip(t - LAG * place[d] - 3 * PIECES, 0, PIECES - 1)
                    out = lax.dynamic_update_slice_in_dim(out, sent[(t, d)], (half - base[d]) + rows * p, axis=0)

        y_out = out.reshape(1, seq_length, width)
        k_cache = k_rot.reshape(1, seq_length, kv_heads, head_dim)
        v_cache = v_loc.reshape(1, seq_length, kv_heads, head_dim)
        return y_out, k_cache, v_cache

    return jax.shard_map(layer_local, mesh=mesh, in_specs=arg_specs, out_specs=out_parts, check_vma=False)
```

```python
import functools

import jax
import jax.numpy as jnp
from jax import lax
from jax.experimental import pallas as pl
from jax.experimental.pallas import tpu as pltpu
from jax.sharding import PartitionSpec as P

EPS = 1e-5
ROPE_BASE = 10000.0
PIECES = 16
PER_GROUP = 4
TILE = 256
QBLK = 256
KBLK = 512

def layer_norm(x_rows, gain_vec):
    x_f32 = x_rows.astype(jnp.float32)
    mean_x = jnp.mean(x_f32, axis=-1, keepdims=True)
    centred = x_f32 - mean_x
    var_x = jnp.mean(centred * centred, axis=-1, keepdims=True)
    return (centred * lax.rsqrt(var_x + EPS) * (1.0 + gain_vec.astype(jnp.float32))).astype(jnp.bfloat16)


def rotary_tables(seq_length, head_dim):
    rot_dims = head_dim // 2
    half_rot = rot_dims // 2
    inv_freq = ROPE_BASE ** (-2.0 * jnp.arange(half_rot, dtype=jnp.float32) / rot_dims)
    angles = jnp.arange(seq_length, dtype=jnp.float32)[:, None] * inv_freq[None, :]
    cos_t, sin_t = jnp.cos(angles), jnp.sin(angles)
    zeros = jnp.zeros_like(sin_t)
    tail = jnp.zeros((seq_length, head_dim - rot_dims), jnp.float32)
    keep = jnp.concatenate([cos_t, cos_t, tail + 1.0], axis=1)
    from_low = jnp.concatenate([zeros, sin_t, tail], axis=1)
    from_high = jnp.concatenate([-sin_t, zeros, tail], axis=1)
    return keep, from_low, from_high


def rotate(t_bf16, keep, from_low, from_high):
    head_dim = t_bf16.shape[1]
    quarter = head_dim // 4
    t_f32 = t_bf16.astype(jnp.float32)
    low = pltpu.roll(t_f32, quarter, 1)
    high = pltpu.roll(t_f32, head_dim - quarter, 1)
    return (t_f32 * keep + low * from_low + high * from_high).astype(jnp.bfloat16)


def attention_kernel(len_ref, q_ref, k_ref, v_ref, qc_ref, ql_ref, qh_ref, kc_ref, kl_ref, kh_ref, ctx_ref, k_rot_ref):
    q_block = pl.program_id(1)
    head_dim = k_ref.shape[1]
    heads = q_ref.shape[1] // head_dim

    @pl.when(q_block == 0)
    def _():
        k_rot_ref[...] = rotate(k_ref[...], kc_ref[...], kl_ref[...], kh_ref[...])

    seq_len = len_ref[0]
    scale = head_dim ** -0.5
    row0 = q_block * QBLK
    n_keys = jnp.minimum(row0 + QBLK, seq_len)
    n_blocks = (n_keys + KBLK - 1) // KBLK
    n_clear = jnp.minimum(row0, seq_len) // KBLK
    tables = (qc_ref[...], ql_ref[...], qh_ref[...])
    q_rot = [rotate(q_ref[:, h * head_dim:(h + 1) * head_dim], *tables) for h in range(heads)]

    def step(masked, kb, carry):
        start = pl.multiple_of(kb * KBLK, KBLK)
        k_blk = k_rot_ref[pl.ds(start, KBLK), :]
        v_blk = v_ref[pl.ds(start, KBLK), :]
        if masked:
            rows = row0 + lax.broadcasted_iota(jnp.int32, (QBLK, KBLK), 0)
            cols = start + lax.broadcasted_iota(jnp.int32, (QBLK, KBLK), 1)
            allowed = (cols <= rows) & (cols < seq_len)
        out = []
        for h in range(heads):
            m_old, l_old, acc = carry[h]
            s = lax.dot_general(q_rot[h], k_blk, (((1,), (1,)), ((), ())), preferred_element_type=jnp.float32) * scale
            if masked:
                s = jnp.where(allowed, s, -1e30)
            m_new = jnp.maximum(m_old, jnp.max(s, axis=1, keepdims=True))
            corr = jnp.exp(m_old - m_new)
            p = jnp.exp(s - m_new)
            l_new = l_old * corr + jnp.sum(p, axis=1, keepdims=True)
            acc = acc * corr + jnp.dot(p.astype(jnp.bfloat16), v_blk, preferred_element_type=jnp.float32)
            out.append((m_new, l_new, acc))
        return tuple(out)

    init = tuple(
        (jnp.full((QBLK, 1), -1e30, jnp.float32), jnp.zeros((QBLK, 1), jnp.float32), jnp.zeros((QBLK, head_dim), jnp.float32))
        for _ in range(heads)
    )
    carry = lax.fori_loop(0, n_clear, functools.partial(step, False), init)
    carry = lax.fori_loop(n_clear, n_blocks, functools.partial(step, True), carry)
    for h in range(heads):
        _, l_sum, acc = carry[h]
        ctx_ref[:, h * head_dim:(h + 1) * head_dim] = (acc / l_sum).astype(jnp.bfloat16)


def attend(qkv, seq_lens, tables, q_heads, kv_heads, head_dim):
    seq_length = qkv.shape[0]
    group = q_heads // kv_heads
    width = group * head_dim
    table_q = pl.BlockSpec((QBLK, head_dim), lambda g, i, *_: (i, 0))
    table_k = pl.BlockSpec((seq_length, head_dim), lambda g, i, *_: (0, 0))
    pairs = 4 * q_heads * head_dim * seq_length * seq_length // 2
    return pl.pallas_call(
        attention_kernel,
        grid_spec=pltpu.PrefetchScalarGridSpec(
            num_scalar_prefetch=1,
            grid=(kv_heads, seq_length // QBLK),
            in_specs=[
                pl.BlockSpec((QBLK, width), lambda g, i, *_: (i, g)),
                pl.BlockSpec((seq_length, head_dim), lambda g, i, *_: (0, q_heads + g)),
                pl.BlockSpec((seq_length, head_dim), lambda g, i, *_: (0, q_heads + kv_heads + g)),
                table_q, table_q, table_q, table_k, table_k, table_k,
            ],
            out_specs=[
                pl.BlockSpec((QBLK, width), lambda g, i, *_: (i, g)),
                pl.BlockSpec((seq_length, head_dim), lambda g, i, *_: (0, g)),
            ],
        ),
        out_shape=[
            jax.ShapeDtypeStruct((seq_length, q_heads * head_dim), jnp.bfloat16),
            jax.ShapeDtypeStruct((seq_length, kv_heads * head_dim), jnp.bfloat16),
        ],
        compiler_params=pltpu.CompilerParams(dimension_semantics=("arbitrary", "arbitrary"), vmem_limit_bytes=48 << 20),
        cost_estimate=pl.CostEstimate(flops=pairs, bytes_accessed=16 << 20, transcendentals=q_heads * seq_length * seq_length // 2),
        name="attend",
    )(seq_lens, qkv, qkv, qkv, *tables, *tables)


class Line:
    def __init__(self, n_tp, half):
        self.z = lax.axis_index("tp")
        self.others = (lax.axis_index("dp"), lax.axis_index("fsdp"))
        self.last = n_tp - 1
        self.place = (self.z, self.last - self.z)
        self.sum_base = (half, 0)
        self.row_base = (0, half)

    def device(self, d):
        return (self.others[0], self.z + (1 if d == 0 else -1), self.others[1])

    def copy(self, d, src, dst, send_sem, recv_sem):
        return pltpu.make_async_remote_copy(
            src_ref=src, dst_ref=dst, send_sem=send_sem, recv_sem=recv_sem,
            device_id=self.device(d), device_id_type=pl.DeviceIdType.MESH,
        )

    def meet(self):
        barrier = pltpu.get_barrier_semaphore()
        for d in range(2):

            @pl.when(self.place[d] < self.last)
            def _():
                pl.semaphore_signal(barrier, inc=1, device_id=self.device(d), device_id_type=pl.DeviceIdType.MESH)

        pl.semaphore_wait(barrier, sum((place < self.last).astype(jnp.int32) for place in self.place))


def own_copies(line, half, pairs):
    for d in range(2):

        @pl.when(line.place[d] == line.last)
        def _():
            pairs(d, line.sum_base[d])


def sum_step(line, d, p, rows, part_ref, sum_ref, send, recv, finish):
    here = pl.ds(pl.multiple_of(p * rows, rows), rows)
    part_rows = pl.ds(pl.multiple_of(line.sum_base[d] + p * rows, rows), rows)
    place = line.place[d]

    @pl.when(place == 0)
    def _():
        line.copy(d, part_ref.at[part_rows], sum_ref.at[d, here], send.at[d, p], recv.at[d, p]).start()

    @pl.when(place > 0)
    def _():
        copy = line.copy(d, sum_ref.at[d, here], sum_ref.at[d, here], send.at[d, p], recv.at[d, p])
        copy.wait_recv()
        total = sum_ref[d, here, :].astype(jnp.float32) + part_ref[part_rows, :].astype(jnp.float32)

        @pl.when(place < line.last)
        def _():
            sum_ref[d, here, :] = total.astype(jnp.bfloat16)
            copy.start()

        @pl.when(place == line.last)
        def _():
            rows_done = (sum_ref[1 - d, here, :].astype(jnp.float32) + total).astype(jnp.bfloat16)
            sum_ref[d, here, :] = rows_done
            finish(here, part_rows, rows_done)


def drain_sums(line, rows, part_ref, sum_ref, send, recv, finished):
    def body(p, _):
        here = pl.ds(pl.multiple_of(p * rows, rows), rows)
        for d in range(2):

            @pl.when(line.place[d] < line.last)
            def _():
                line.copy(d, sum_ref.at[d, here], sum_ref.at[d, here], send.at[d, p], recv.at[d, p]).wait_send()

            @pl.when(line.place[d] == line.last)
            def _():
                finished(d, p, here)

        return 0

    lax.fori_loop(0, PIECES, body, 0)


def reduce_kernel(n_tp, part_hbm, x_hbm, gain_ref, x_own_hbm, h_own_hbm, part, sums, part_sem, x_sem, send, recv, x_out, h_out):
    half = part.shape[0] // 2
    rows = half // PIECES
    line = Line(n_tp, half)
    load = pltpu.make_async_copy(part_hbm, part, part_sem)
    load.start()

    def own(d, row):
        return pltpu.make_async_copy(x_hbm.at[pl.ds(row, half)], sums.at[1 - d], x_sem)

    own_copies(line, half, lambda d, row: own(d, row).start())
    line.meet()
    own_copies(line, half, lambda d, row: own(d, row).wait())
    load.wait()

    def outward(d, p, here):
        part_rows = pl.ds(pl.multiple_of(line.sum_base[d] + p * rows, rows), rows)
        return (
            pltpu.make_async_copy(sums.at[d, here], x_own_hbm.at[here], x_out.at[p]),
            pltpu.make_async_copy(part.at[part_rows], h_own_hbm.at[here], h_out.at[p]),
        )

    def step(t, _):
        for d in range(2):
            p = t - line.place[d]

            def finish(here, part_rows, rows_done, d=d, p=p):
                part[part_rows, :] = layer_norm(rows_done, gain_ref[...])
                for copy in outward(d, p, here):
                    copy.start()

            @pl.when((p >= 0) & (p < PIECES))
            def _():
                sum_step(line, d, p, rows, part, sums, send, recv, finish)

        return 0

    lax.fori_loop(0, PIECES + line.last, step, 0)

    def finished(d, p, here):
        for copy in outward(d, p, here):
            copy.wait()

    drain_sums(line, rows, part, sums, send, recv, finished)


def mlp_kernel(n_tp, x_own_hbm, h_own_hbm, up_hbm, down_hbm, out_hbm, up, down, h, sums, act,
               w_sem, own_sem, h_send, h_recv, send, recv, y_send, y_recv, y_out):
    half = h.shape[0] // 2
    rows = half // PIECES
    group_rows = rows * PER_GROUP
    groups = PIECES // PER_GROUP
    up_tiles, down_tiles = up.shape[1] // TILE, down.shape[1] // TILE
    per_step = pl.cdiv(up_tiles + down_tiles, PER_GROUP)
    line = Line(n_tp, half)
    first = PER_GROUP + line.last
    loads = (pltpu.make_async_copy(up_hbm, up, w_sem.at[0]), pltpu.make_async_copy(down_hbm, down, w_sem.at[1]))

    def own(d, row):
        return (
            pltpu.make_async_copy(x_own_hbm, sums.at[1 - d], own_sem.at[0]),
            pltpu.make_async_copy(h_own_hbm, h.at[pl.ds(row, half)], own_sem.at[1]),
        )

    own_copies(line, half, lambda d, row: [c.start() for c in own(d, row)])
    for load in loads:
        load.start()
    line.meet()
    own_copies(line, half, lambda d, row: [c.wait() for c in own(d, row)])

    def row_slice(d, p):
        return pl.ds(pl.multiple_of(line.row_base[d] + p * rows, rows), rows)

    def h_copy(d, p):
        return line.copy(d, h.at[row_slice(d, p)], h.at[row_slice(d, p)], h_send.at[d, p], h_recv.at[d, p])

    def y_local(d, p, here):
        return pltpu.make_async_copy(sums.at[d, here], out_hbm.at[row_slice(1 - d, p)], y_out.at[p])

    def y_first(d, p):
        here = pl.ds(pl.multiple_of(p * rows, rows), rows)
        return line.copy(d, sums.at[1 - d, here], out_hbm.at[row_slice(d, p)], y_send.at[d, p], y_recv.at[d, p])

    def y_next(d, p):
        return line.copy(d, out_hbm.at[row_slice(d, p)], out_hbm.at[row_slice(d, p)], y_send.at[d, p], y_recv.at[d, p])

    def group_slices(g):
        return [pl.ds(pl.multiple_of(base + g * group_rows, group_rows), group_rows) for base in (0, half)]

    def product(g, unit):
        @pl.when(unit < up_tiles)
        def _():
            lanes = pl.ds(pl.multiple_of(unit * TILE, TILE), TILE)
            for k, group in enumerate(group_slices(g)):
                pre = jnp.dot(h[group, :], up[:, lanes], preferred_element_type=jnp.float32)
                act[k * group_rows:(k + 1) * group_rows, lanes] = jnp.square(jnp.maximum(pre, 0.0)).astype(jnp.bfloat16)

        @pl.when(unit == up_tiles)
        def _():
            for q in range(PER_GROUP):
                for d in range(2):

                    @pl.when(line.place[d] < line.last)
                    def _():
                        h_copy(d, g * PER_GROUP + q).wait_send()

        @pl.when((unit >= up_tiles) & (unit < up_tiles + down_tiles))
        def _():
            lanes = pl.ds(pl.multiple_of((unit - up_tiles) * TILE, TILE), TILE)
            for k, group in enumerate(group_slices(g)):
                part = jnp.dot(act[k * group_rows:(k + 1) * group_rows, :], down[:, lanes], preferred_element_type=jnp.float32)
                h[group, lanes] = part.astype(jnp.bfloat16)

    def step(t, _):
        for d in range(2):
            place = line.place[d]
            m = t - place

            @pl.when((m >= 0) & (m < PIECES))
            def _():
                @pl.when(place > 0)
                def _():
                    h_copy(d, m).wait_recv()

                @pl.when(place < line.last)
                def _():
                    h_copy(d, m).start()

            p = m - PIECES

            def finish(here, part_rows, rows_done, d=d, p=p):
                y_local(d, p, here).start()

            @pl.when((p >= 0) & (p < PIECES))
            def _():
                sum_step(line, d, p, rows, h, sums, send, recv, finish)

            q = m - 2 * PIECES

            @pl.when((q >= 0) & (q < PIECES))
            def _():
                @pl.when(place == 0)
                def _():
                    y_first(d, q).start()

                @pl.when(place > 0)
                def _():
                    y_next(d, q).wait_recv()

                    @pl.when(place < line.last)
                    def _():
                        y_next(d, q).start()

        @pl.when(t == first)
        def _():
            for load in loads:
                load.wait()

        k = t - first

        @pl.when((k >= 0) & (k < PIECES))
        def _():
            def units(u, _):
                product(k // PER_GROUP, (k % PER_GROUP) * per_step + u)
                return 0

            lax.fori_loop(0, per_step, units, 0)

        return 0

    lax.fori_loop(0, 3 * PIECES + line.last, step, 0)
    drain_sums(line, rows, h, sums, send, recv, lambda d, p, here: y_local(d, p, here).wait())

    def drain(p, _):
        for d in range(2):

            @pl.when(line.place[d] < line.last)
            def _():
                y_next(d, p).wait_send()

        return 0

    lax.fori_loop(0, PIECES, drain, 0)


def reduce_rows(n_tp, part, x_rows, gain):
    seq_length, width = part.shape
    half = seq_length // 2
    own = jax.ShapeDtypeStruct((half, width), jnp.bfloat16)
    any_spec = pl.BlockSpec(memory_space=pl.ANY)
    dma = pltpu.SemaphoreType.DMA
    return pl.pallas_call(
        functools.partial(reduce_kernel, n_tp),
        in_specs=[any_spec, any_spec, pl.BlockSpec(memory_space=pltpu.VMEM)],
        out_specs=[any_spec, any_spec],
        out_shape=[own, own],
        scratch_shapes=[
            pltpu.VMEM((seq_length, width), jnp.bfloat16),
            pltpu.VMEM((2, half, width), jnp.bfloat16),
            dma, dma, dma((2, PIECES)), dma((2, PIECES)), dma((PIECES,)), dma((PIECES,)),
        ],
        compiler_params=pltpu.CompilerParams(collective_id=0, has_side_effects=True, vmem_limit_bytes=40 << 20),
        cost_estimate=pl.CostEstimate(flops=150 * 10 ** 9, bytes_accessed=32 << 20, transcendentals=0),
        name="reduce_rows",
    )(part, x_rows, gain.reshape(1, width))


def mlp_rows(n_tp, x_own, h_own, up_full, down_full):
    half, width = x_own.shape
    hidden = up_full.shape[1]
    any_spec = pl.BlockSpec(memory_space=pl.ANY)
    dma = pltpu.SemaphoreType.DMA
    return pl.pallas_call(
        functools.partial(mlp_kernel, n_tp),
        in_specs=[any_spec] * 4,
        out_specs=any_spec,
        out_shape=jax.ShapeDtypeStruct((2 * half, width), jnp.bfloat16),
        scratch_shapes=[
            pltpu.VMEM((width, hidden), jnp.bfloat16),
            pltpu.VMEM((hidden, width), jnp.bfloat16),
            pltpu.VMEM((2 * half, width), jnp.bfloat16),
            pltpu.VMEM((2, half, width), jnp.bfloat16),
            pltpu.VMEM((2 * half // PIECES * PER_GROUP, hidden), jnp.bfloat16),
            dma((2,)), dma((2,)),
        ] + [dma((2, PIECES))] * 6 + [dma((PIECES,))],
        compiler_params=pltpu.CompilerParams(collective_id=1, has_side_effects=True, vmem_limit_bytes=63 << 20),
        cost_estimate=pl.CostEstimate(flops=400 * 10 ** 9, bytes_accessed=64 << 20, transcendentals=0),
        name="mlp_rows",
    )(x_own, h_own, up_full, down_full)


def solution(mesh):
    batch_axes = ("dp", "fsdp")
    arg_specs = (P(batch_axes, None, None), P(batch_axes), P(None), P("fsdp", "tp", None), P("fsdp", "tp", None), P("fsdp", "tp", None), P("tp", None, "fsdp"), P(None), P("fsdp", "tp"), P("tp", "fsdp"))
    out_parts = (P(batch_axes, None, None), P(batch_axes, None, "tp", None), P(batch_axes, None, "tp", None))
    n_tp = mesh.shape["tp"]

    def layer_local(x_in, seq_lens, ln1_gain, w_q, w_k, w_v, w_o, ln2_gain, w_up, w_down):
        _, seq_length, width = x_in.shape
        q_heads, kv_heads, head_dim = w_q.shape[1], w_k.shape[1], w_k.shape[2]
        x_rows = x_in.reshape(seq_length, width)

        w_qkv = jnp.concatenate([w.reshape(w.shape[0], -1) for w in (w_q, w_k, w_v)], axis=1)
        qkv_full = lax.all_gather(w_qkv, "fsdp", axis=0, tiled=True)
        o_full = lax.all_gather(w_o.reshape(q_heads * head_dim, -1), "fsdp", axis=1, tiled=True)
        up_full = lax.all_gather(w_up, "fsdp", axis=0, tiled=True)
        down_full = lax.all_gather(w_down, "fsdp", axis=1, tiled=True)

        tables = rotary_tables(seq_length, head_dim)
        h_norm = layer_norm(x_rows, ln1_gain)
        qkv = jnp.dot(h_norm, qkv_full, preferred_element_type=jnp.float32).astype(jnp.bfloat16)
        ctx, k_rot = attend(qkv, seq_lens, tables, q_heads, kv_heads, head_dim)
        v_loc = qkv[:, (q_heads + kv_heads) * head_dim:]
        o_part = jnp.dot(ctx, o_full, preferred_element_type=jnp.float32).astype(jnp.bfloat16)
        x_own, h_own = reduce_rows(n_tp, o_part, x_rows, ln2_gain)
        out = mlp_rows(n_tp, x_own, h_own, up_full, down_full)

        y_out = out.reshape(1, seq_length, width)
        k_cache = k_rot.reshape(1, seq_length, kv_heads, head_dim)
        v_cache = v_loc.reshape(1, seq_length, kv_heads, head_dim)
        return y_out, k_cache, v_cache

    return jax.shard_map(layer_local, mesh=mesh, in_specs=arg_specs, out_specs=out_parts, check_vma=False)
```

```python
import functools

import jax
import jax.numpy as jnp
from jax import lax
from jax.experimental import pallas as pl
from jax.experimental.pallas import tpu as pltpu
from jax.sharding import PartitionSpec as P

EPS = 1e-5
ROPE_BASE = 10000.0
PIECES = 16
PER_GROUP = 4
TILE = 256
QBLK = 256
KBLK = 512

def layer_norm(x_rows, gain_vec):
    x_f32 = x_rows.astype(jnp.float32)
    mean_x = jnp.mean(x_f32, axis=-1, keepdims=True)
    centred = x_f32 - mean_x
    var_x = jnp.mean(centred * centred, axis=-1, keepdims=True)
    return (centred * lax.rsqrt(var_x + EPS) * (1.0 + gain_vec.astype(jnp.float32))).astype(jnp.bfloat16)


def rotary_tables(seq_length, head_dim):
    rot_dims = head_dim // 2
    half_rot = rot_dims // 2
    inv_freq = ROPE_BASE ** (-2.0 * jnp.arange(half_rot, dtype=jnp.float32) / rot_dims)
    angles = jnp.arange(seq_length, dtype=jnp.float32)[:, None] * inv_freq[None, :]
    cos_t, sin_t = jnp.cos(angles), jnp.sin(angles)
    zeros = jnp.zeros_like(sin_t)
    tail = jnp.zeros((seq_length, head_dim - rot_dims), jnp.float32)
    keep = jnp.concatenate([cos_t, cos_t, tail + 1.0], axis=1)
    from_low = jnp.concatenate([zeros, sin_t, tail], axis=1)
    from_high = jnp.concatenate([-sin_t, zeros, tail], axis=1)
    return keep, from_low, from_high


def rotate(t_bf16, keep, from_low, from_high):
    head_dim = t_bf16.shape[1]
    quarter = head_dim // 4
    t_f32 = t_bf16.astype(jnp.float32)
    low = pltpu.roll(t_f32, quarter, 1)
    high = pltpu.roll(t_f32, head_dim - quarter, 1)
    return (t_f32 * keep + low * from_low + high * from_high).astype(jnp.bfloat16)


def strip_attention(q_rot, k_blocks, v_blocks, row0, seq_len):
    head_dim = q_rot[0].shape[1]
    scale = head_dim ** -0.5

    def step(diagonal, kb, carry):
        start = pl.multiple_of(kb * KBLK, KBLK)
        k_blk = k_blocks(start)
        v_blk = v_blocks(start)
        length_bias = jnp.where(start + lax.broadcasted_iota(jnp.int32, (1, KBLK), 1) < seq_len, 0.0, -1e30)
        if diagonal:
            rows = row0 + lax.broadcasted_iota(jnp.int32, (QBLK, KBLK), 0)
            cols = start + lax.broadcasted_iota(jnp.int32, (QBLK, KBLK), 1)
            causal = cols <= rows
        out = []
        for q_head, (m_old, l_old, acc) in zip(q_rot, carry):
            s = lax.dot_general(q_head, k_blk, (((1,), (1,)), ((), ())), preferred_element_type=jnp.float32) * scale + length_bias
            if diagonal:
                s = jnp.where(causal, s, -1e30)
            m_new = jnp.maximum(m_old, jnp.max(s, axis=1, keepdims=True))
            corr = jnp.exp(m_old - m_new)
            p = jnp.exp(s - m_new)
            l_new = l_old * corr + jnp.sum(p, axis=1, keepdims=True)
            acc = acc * corr + jnp.dot(p.astype(jnp.bfloat16), v_blk, preferred_element_type=jnp.float32)
            out.append((m_new, l_new, acc))
        return tuple(out)

    carry = tuple(
        (jnp.full((QBLK, 1), -1e30, jnp.float32), jnp.zeros((QBLK, 1), jnp.float32), jnp.zeros((QBLK, head_dim), jnp.float32))
        for _ in q_rot
    )
    carry = lax.fori_loop(0, row0 // KBLK, functools.partial(step, False), carry)
    carry = lax.fori_loop(row0 // KBLK, (row0 + QBLK + KBLK - 1) // KBLK, functools.partial(step, True), carry)
    return [(acc / l_sum).astype(jnp.bfloat16) for _, l_sum, acc in carry]


def first_strips_kernel(len_ref, q_ref, k_ref, v_ref, qc_ref, ql_ref, qh_ref, kc_ref, kl_ref, kh_ref, ctx_ref, k_rot_ref):
    head_dim = k_ref.shape[1]

    @pl.when(pl.program_id(1) == 0)
    def _():
        k_rot_ref[...] = rotate(k_ref[...], kc_ref[...], kl_ref[...], kh_ref[...])

    tables = (qc_ref[...], ql_ref[...], qh_ref[...])
    heads = range(0, q_ref.shape[1], head_dim)
    context = strip_attention(
        [rotate(q_ref[:, h:h + head_dim], *tables) for h in heads],
        lambda start: k_rot_ref[pl.ds(start, KBLK), :],
        lambda start: v_ref[pl.ds(start, KBLK), :],
        pl.program_id(1) * (k_ref.shape[0] // 2),
        len_ref[0],
    )
    for h, rows in zip(heads, context):
        ctx_ref[:, h:h + head_dim] = rows


def first_strips(qkv, seq_lens, tables, q_heads, kv_heads, head_dim):
    seq_length = qkv.shape[0]
    width = q_heads // kv_heads * head_dim
    strips = seq_length // 2 // QBLK
    table_q = pl.BlockSpec((QBLK, head_dim), lambda g, i, *_: (i * strips, 0))
    table_k = pl.BlockSpec((seq_length, head_dim), lambda g, i, *_: (0, 0))
    return pl.pallas_call(
        first_strips_kernel,
        grid_spec=pltpu.PrefetchScalarGridSpec(
            num_scalar_prefetch=1,
            grid=(kv_heads, 2),
            in_specs=[
                pl.BlockSpec((QBLK, width), lambda g, i, *_: (i * strips, g)),
                pl.BlockSpec((seq_length, head_dim), lambda g, i, *_: (0, q_heads + g)),
                pl.BlockSpec((seq_length, head_dim), lambda g, i, *_: (0, q_heads + kv_heads + g)),
            ] + [table_q] * 3 + [table_k] * 3,
            out_specs=[
                pl.BlockSpec((QBLK, width), lambda g, i, *_: (i, g)),
                pl.BlockSpec((seq_length, head_dim), lambda g, i, *_: (0, g)),
            ],
        ),
        out_shape=[
            jax.ShapeDtypeStruct((2 * QBLK, q_heads * head_dim), jnp.bfloat16),
            jax.ShapeDtypeStruct((seq_length, kv_heads * head_dim), jnp.bfloat16),
        ],
        compiler_params=pltpu.CompilerParams(dimension_semantics=("arbitrary", "arbitrary"), vmem_limit_bytes=48 << 20),
        cost_estimate=pl.CostEstimate(flops=15 * 10 ** 9, bytes_accessed=12 << 20, transcendentals=0),
        name="first_strips",
    )(seq_lens, qkv, qkv, qkv, *tables, *tables)


class Line:
    def __init__(self, n_tp, half):
        self.z = lax.axis_index("tp")
        self.others = (lax.axis_index("dp"), lax.axis_index("fsdp"))
        self.last = n_tp - 1
        self.place = (self.z, self.last - self.z)
        self.sum_base = (half, 0)
        self.row_base = (0, half)

    def device(self, d):
        return (self.others[0], self.z + (1 if d == 0 else -1), self.others[1])

    def copy(self, d, src, dst, send_sem, recv_sem):
        return pltpu.make_async_remote_copy(
            src_ref=src, dst_ref=dst, send_sem=send_sem, recv_sem=recv_sem,
            device_id=self.device(d), device_id_type=pl.DeviceIdType.MESH,
        )

    def meet(self):
        barrier = pltpu.get_barrier_semaphore()
        for d in range(2):

            @pl.when(self.place[d] < self.last)
            def _():
                pl.semaphore_signal(barrier, inc=1, device_id=self.device(d), device_id_type=pl.DeviceIdType.MESH)

        pl.semaphore_wait(barrier, sum((place < self.last).astype(jnp.int32) for place in self.place))


def own_copies(line, half, pairs):
    for d in range(2):

        @pl.when(line.place[d] == line.last)
        def _():
            pairs(d, line.sum_base[d])


def sum_step(line, d, p, rows, part_ref, sum_ref, send, recv, finish):
    here = pl.ds(pl.multiple_of(p * rows, rows), rows)
    part_rows = pl.ds(pl.multiple_of(line.sum_base[d] + p * rows, rows), rows)
    place = line.place[d]

    @pl.when(place == 0)
    def _():
        line.copy(d, part_ref.at[part_rows], sum_ref.at[d, here], send.at[d, p], recv.at[d, p]).start()

    @pl.when(place > 0)
    def _():
        copy = line.copy(d, sum_ref.at[d, here], sum_ref.at[d, here], send.at[d, p], recv.at[d, p])
        copy.wait_recv()
        total = sum_ref[d, here, :].astype(jnp.float32) + part_ref[part_rows, :].astype(jnp.float32)

        @pl.when(place < line.last)
        def _():
            sum_ref[d, here, :] = total.astype(jnp.bfloat16)
            copy.start()

        @pl.when(place == line.last)
        def _():
            rows_done = (sum_ref[1 - d, here, :].astype(jnp.float32) + total).astype(jnp.bfloat16)
            sum_ref[d, here, :] = rows_done
            finish(here, part_rows, rows_done)


def drain_sums(line, rows, part_ref, sum_ref, send, recv, finished):
    def body(p, _):
        here = pl.ds(pl.multiple_of(p * rows, rows), rows)
        for d in range(2):

            @pl.when(line.place[d] < line.last)
            def _():
                line.copy(d, sum_ref.at[d, here], sum_ref.at[d, here], send.at[d, p], recv.at[d, p]).wait_send()

            @pl.when(line.place[d] == line.last)
            def _():
                finished(d, p, here)

        return 0

    lax.fori_loop(0, PIECES, body, 0)


def attend_reduce_kernel(n_tp, q_heads, len_ref, qkv, k_rot, keep, from_low, from_high, gain_ref, first_hbm, o_hbm, x_hbm,
                         x_own_hbm, h_own_hbm, o_full, part, sums, ctx, load_sem, x_sem, send, recv, x_out, h_out):
    half = part.shape[0] // 2
    rows = half // PIECES
    strips = half // QBLK
    per_strip = PIECES // strips
    head_dim = keep.shape[1]
    kv_heads = k_rot.shape[1] // head_dim
    group = q_heads // kv_heads
    line = Line(n_tp, half)
    loads = (pltpu.make_async_copy(first_hbm, ctx, load_sem.at[0]), pltpu.make_async_copy(o_hbm, o_full, load_sem.at[1]))
    for load in loads:
        load.start()

    def own(d, row):
        return pltpu.make_async_copy(x_hbm.at[pl.ds(row, half)], sums.at[1 - d], x_sem)

    own_copies(line, half, lambda d, row: own(d, row).start())
    line.meet()
    for load in loads:
        load.wait()
    seq_len = len_ref[0]

    def lanes_of(index, size):
        return pl.ds(pl.multiple_of(index * size, size), size)

    def output_product(strip):
        def tile(n, _):
            lanes = lanes_of(n, TILE)
            for k in range(2):
                product = jnp.dot(ctx[k * QBLK:(k + 1) * QBLK, :], o_full[:, lanes], preferred_element_type=jnp.float32)
                part[pl.ds(pl.multiple_of(k * half + strip * QBLK, QBLK), QBLK), lanes] = product.astype(jnp.bfloat16)
            return 0

        lax.fori_loop(0, part.shape[1] // TILE, tile, 0)

    def attend(strip, k, kv):
        row0 = pl.multiple_of(k * half + strip * QBLK, QBLK)
        q_rows = pl.ds(row0, QBLK)
        tables = (keep[q_rows, :], from_low[q_rows, :], from_high[q_rows, :])
        context = strip_attention(
            [rotate(qkv[q_rows, lanes_of(kv * group + h, head_dim)], *tables) for h in range(group)],
            lambda start: k_rot[pl.ds(start, KBLK), lanes_of(kv, head_dim)],
            lambda start: qkv[pl.ds(start, KBLK), lanes_of(q_heads + kv_heads + kv, head_dim)],
            row0,
            seq_len,
        )
        for h in range(group):
            ctx[pl.ds(pl.multiple_of(k * QBLK, QBLK), QBLK), lanes_of(kv * group + h, head_dim)] = context[h]

    output_product(0)
    own_copies(line, half, lambda d, row: own(d, row).wait())

    def outward(d, p, here):
        part_rows = pl.ds(pl.multiple_of(line.sum_base[d] + p * rows, rows), rows)
        return (
            pltpu.make_async_copy(sums.at[d, here], x_own_hbm.at[here], x_out.at[p]),
            pltpu.make_async_copy(part.at[part_rows], h_own_hbm.at[here], h_out.at[p]),
        )

    def step(t, _):
        for d in range(2):
            p = t - line.place[d]

            def finish(here, part_rows, rows_done, d=d, p=p):
                part[part_rows, :] = layer_norm(rows_done, gain_ref[...])
                for copy in outward(d, p, here):
                    copy.start()

            @pl.when((p >= 0) & (p < PIECES))
            def _():
                sum_step(line, d, p, rows, part, sums, send, recv, finish)

        strip = t // per_strip + 1
        unit = t % per_strip

        @pl.when(strip < strips)
        def _():
            @pl.when(unit < 2 * kv_heads)
            def _():
                attend(strip, unit // kv_heads, unit % kv_heads)

            @pl.when(unit == per_strip - 1)
            def _():
                output_product(strip)

        return 0

    lax.fori_loop(0, PIECES + line.last, step, 0)

    def finished(d, p, here):
        for copy in outward(d, p, here):
            copy.wait()

    drain_sums(line, rows, part, sums, send, recv, finished)


def mlp_kernel(n_tp, x_own_hbm, h_own_hbm, up_hbm, down_hbm, out_hbm, up, down, h, sums, act,
               w_sem, own_sem, h_send, h_recv, send, recv, y_send, y_recv, y_out):
    half = h.shape[0] // 2
    rows = half // PIECES
    group_rows = rows * PER_GROUP
    groups = PIECES // PER_GROUP
    up_tiles, down_tiles = up.shape[1] // TILE, down.shape[1] // TILE
    per_step = pl.cdiv(up_tiles + down_tiles, PER_GROUP)
    line = Line(n_tp, half)
    first = PER_GROUP + line.last
    loads = (pltpu.make_async_copy(up_hbm, up, w_sem.at[0]), pltpu.make_async_copy(down_hbm, down, w_sem.at[1]))

    def own(d, row):
        return (
            pltpu.make_async_copy(x_own_hbm, sums.at[1 - d], own_sem.at[0]),
            pltpu.make_async_copy(h_own_hbm, h.at[pl.ds(row, half)], own_sem.at[1]),
        )

    own_copies(line, half, lambda d, row: [c.start() for c in own(d, row)])
    for load in loads:
        load.start()
    line.meet()
    own_copies(line, half, lambda d, row: [c.wait() for c in own(d, row)])

    def row_slice(d, p):
        return pl.ds(pl.multiple_of(line.row_base[d] + p * rows, rows), rows)

    def h_copy(d, p):
        return line.copy(d, h.at[row_slice(d, p)], h.at[row_slice(d, p)], h_send.at[d, p], h_recv.at[d, p])

    def y_local(d, p, here):
        return pltpu.make_async_copy(sums.at[d, here], out_hbm.at[row_slice(1 - d, p)], y_out.at[p])

    def y_first(d, p):
        here = pl.ds(pl.multiple_of(p * rows, rows), rows)
        return line.copy(d, sums.at[1 - d, here], out_hbm.at[row_slice(d, p)], y_send.at[d, p], y_recv.at[d, p])

    def y_next(d, p):
        return line.copy(d, out_hbm.at[row_slice(d, p)], out_hbm.at[row_slice(d, p)], y_send.at[d, p], y_recv.at[d, p])

    def group_slices(g):
        return [pl.ds(pl.multiple_of(base + g * group_rows, group_rows), group_rows) for base in (0, half)]

    def product(g, unit):
        @pl.when(unit < up_tiles)
        def _():
            lanes = pl.ds(pl.multiple_of(unit * TILE, TILE), TILE)
            for k, group in enumerate(group_slices(g)):
                pre = jnp.dot(h[group, :], up[:, lanes], preferred_element_type=jnp.float32)
                act[k * group_rows:(k + 1) * group_rows, lanes] = jnp.square(jnp.maximum(pre, 0.0)).astype(jnp.bfloat16)

        @pl.when(unit == up_tiles)
        def _():
            for q in range(PER_GROUP):
                for d in range(2):

                    @pl.when(line.place[d] < line.last)
                    def _():
                        h_copy(d, g * PER_GROUP + q).wait_send()

        @pl.when((unit >= up_tiles) & (unit < up_tiles + down_tiles))
        def _():
            lanes = pl.ds(pl.multiple_of((unit - up_tiles) * TILE, TILE), TILE)
            for k, group in enumerate(group_slices(g)):
                part = jnp.dot(act[k * group_rows:(k + 1) * group_rows, :], down[:, lanes], preferred_element_type=jnp.float32)
                h[group, lanes] = part.astype(jnp.bfloat16)

    def step(t, _):
        for d in range(2):
            place = line.place[d]
            m = t - place

            @pl.when((m >= 0) & (m < PIECES))
            def _():
                @pl.when(place > 0)
                def _():
                    h_copy(d, m).wait_recv()

                @pl.when(place < line.last)
                def _():
                    h_copy(d, m).start()

            p = m - PIECES

            def finish(here, part_rows, rows_done, d=d, p=p):
                y_local(d, p, here).start()

            @pl.when((p >= 0) & (p < PIECES))
            def _():
                sum_step(line, d, p, rows, h, sums, send, recv, finish)

            q = m - 2 * PIECES

            @pl.when((q >= 0) & (q < PIECES))
            def _():
                @pl.when(place == 0)
                def _():
                    y_first(d, q).start()

                @pl.when(place > 0)
                def _():
                    y_next(d, q).wait_recv()

                    @pl.when(place < line.last)
                    def _():
                        y_next(d, q).start()

        @pl.when(t == first)
        def _():
            for load in loads:
                load.wait()

        k = t - first

        @pl.when((k >= 0) & (k < PIECES))
        def _():
            def units(u, _):
                product(k // PER_GROUP, (k % PER_GROUP) * per_step + u)
                return 0

            lax.fori_loop(0, per_step, units, 0)

        return 0

    lax.fori_loop(0, 3 * PIECES + line.last, step, 0)
    drain_sums(line, rows, h, sums, send, recv, lambda d, p, here: y_local(d, p, here).wait())

    def drain(p, _):
        for d in range(2):

            @pl.when(line.place[d] < line.last)
            def _():
                y_next(d, p).wait_send()

        return 0

    lax.fori_loop(0, PIECES, drain, 0)


def attend_reduce(n_tp, q_heads, seq_lens, qkv, k_rot, tables, gain, first_ctx, o_full, x_rows):
    seq_length, width = x_rows.shape
    half = seq_length // 2
    own = jax.ShapeDtypeStruct((half, width), jnp.bfloat16)
    any_spec = pl.BlockSpec(memory_space=pl.ANY)
    vmem_spec = pl.BlockSpec(memory_space=pltpu.VMEM)
    dma = pltpu.SemaphoreType.DMA
    return pl.pallas_call(
        functools.partial(attend_reduce_kernel, n_tp, q_heads),
        in_specs=[pl.BlockSpec(memory_space=pltpu.SMEM)] + [vmem_spec] * 6 + [any_spec] * 3,
        out_specs=[any_spec, any_spec],
        out_shape=[own, own],
        scratch_shapes=[
            pltpu.VMEM(o_full.shape, jnp.bfloat16),
            pltpu.VMEM((seq_length, width), jnp.bfloat16),
            pltpu.VMEM((2, half, width), jnp.bfloat16),
            pltpu.VMEM(first_ctx.shape, jnp.bfloat16),
            dma((2,)), dma, dma((2, PIECES)), dma((2, PIECES)), dma((PIECES,)), dma((PIECES,)),
        ],
        compiler_params=pltpu.CompilerParams(collective_id=0, has_side_effects=True, vmem_limit_bytes=60 << 20),
        cost_estimate=pl.CostEstimate(flops=150 * 10 ** 9, bytes_accessed=32 << 20, transcendentals=0),
        name="attend_reduce",
    )(seq_lens, qkv, k_rot, *tables, gain.reshape(1, width), first_ctx, o_full, x_rows)


def mlp_rows(n_tp, x_own, h_own, up_full, down_full):
    half, width = x_own.shape
    hidden = up_full.shape[1]
    any_spec = pl.BlockSpec(memory_space=pl.ANY)
    dma = pltpu.SemaphoreType.DMA
    return pl.pallas_call(
        functools.partial(mlp_kernel, n_tp),
        in_specs=[any_spec] * 4,
        out_specs=any_spec,
        out_shape=jax.ShapeDtypeStruct((2 * half, width), jnp.bfloat16),
        scratch_shapes=[
            pltpu.VMEM((width, hidden), jnp.bfloat16),
            pltpu.VMEM((hidden, width), jnp.bfloat16),
            pltpu.VMEM((2 * half, width), jnp.bfloat16),
            pltpu.VMEM((2, half, width), jnp.bfloat16),
            pltpu.VMEM((2 * half // PIECES * PER_GROUP, hidden), jnp.bfloat16),
            dma((2,)), dma((2,)),
        ] + [dma((2, PIECES))] * 6 + [dma((PIECES,))],
        compiler_params=pltpu.CompilerParams(collective_id=1, has_side_effects=True, vmem_limit_bytes=63 << 20),
        cost_estimate=pl.CostEstimate(flops=400 * 10 ** 9, bytes_accessed=64 << 20, transcendentals=0),
        name="mlp_rows",
    )(x_own, h_own, up_full, down_full)


def solution(mesh):
    batch_axes = ("dp", "fsdp")
    arg_specs = (P(batch_axes, None, None), P(batch_axes), P(None), P("fsdp", "tp", None), P("fsdp", "tp", None), P("fsdp", "tp", None), P("tp", None, "fsdp"), P(None), P("fsdp", "tp"), P("tp", "fsdp"))
    out_parts = (P(batch_axes, None, None), P(batch_axes, None, "tp", None), P(batch_axes, None, "tp", None))
    n_tp = mesh.shape["tp"]

    def layer_local(x_in, seq_lens, ln1_gain, w_q, w_k, w_v, w_o, ln2_gain, w_up, w_down):
        _, seq_length, width = x_in.shape
        q_heads, kv_heads, head_dim = w_q.shape[1], w_k.shape[1], w_k.shape[2]
        x_rows = x_in.reshape(seq_length, width)

        w_qkv = jnp.concatenate([w.reshape(w.shape[0], -1) for w in (w_q, w_k, w_v)], axis=1)
        qkv_full = lax.all_gather(w_qkv, "fsdp", axis=0, tiled=True)
        o_full = lax.all_gather(w_o.reshape(q_heads * head_dim, -1), "fsdp", axis=1, tiled=True)
        up_full = lax.all_gather(w_up, "fsdp", axis=0, tiled=True)
        down_full = lax.all_gather(w_down, "fsdp", axis=1, tiled=True)

        tables = rotary_tables(seq_length, head_dim)
        h_norm = layer_norm(x_rows, ln1_gain)
        qkv = jnp.dot(h_norm, qkv_full, preferred_element_type=jnp.float32).astype(jnp.bfloat16)
        first_ctx, k_rot = first_strips(qkv, seq_lens, tables, q_heads, kv_heads, head_dim)
        v_loc = qkv[:, (q_heads + kv_heads) * head_dim:]
        x_own, h_own = attend_reduce(n_tp, q_heads, seq_lens, qkv, k_rot, tables, ln2_gain, first_ctx, o_full, x_rows)
        out = mlp_rows(n_tp, x_own, h_own, up_full, down_full)

        y_out = out.reshape(1, seq_length, width)
        k_cache = k_rot.reshape(1, seq_length, kv_heads, head_dim)
        v_cache = v_loc.reshape(1, seq_length, kv_heads, head_dim)
        return y_out, k_cache, v_cache

    return jax.shard_map(layer_local, mesh=mesh, in_specs=arg_specs, out_specs=out_parts, check_vma=False)
```

```python
import functools

import jax
import jax.numpy as jnp
from jax import lax
from jax.experimental import pallas as pl
from jax.experimental.pallas import tpu as pltpu
from jax.sharding import PartitionSpec as P

EPS = 1e-5
ROPE_BASE = 10000.0
LOG2_E = 1.4426950408889634
PIECES = 16
PER_GROUP = 4
TILE = 256
QBLK = 256
KBLK = 512

def layer_norm(x_rows, gain_vec):
    x_f32 = x_rows.astype(jnp.float32)
    mean_x = jnp.mean(x_f32, axis=-1, keepdims=True)
    centred = x_f32 - mean_x
    var_x = jnp.mean(centred * centred, axis=-1, keepdims=True)
    return (centred * lax.rsqrt(var_x + EPS) * (1.0 + gain_vec.astype(jnp.float32))).astype(jnp.bfloat16)


def rotary_tables(seq_length, head_dim):
    rot_dims = head_dim // 2
    half_rot = rot_dims // 2
    inv_freq = ROPE_BASE ** (-2.0 * jnp.arange(half_rot, dtype=jnp.float32) / rot_dims)
    angles = jnp.arange(seq_length, dtype=jnp.float32)[:, None] * inv_freq[None, :]
    cos_t, sin_t = jnp.cos(angles), jnp.sin(angles)
    zeros = jnp.zeros_like(sin_t)
    tail = jnp.zeros((seq_length, head_dim - rot_dims), jnp.float32)
    keep = jnp.concatenate([cos_t, cos_t, tail + 1.0], axis=1)
    from_low = jnp.concatenate([zeros, sin_t, tail], axis=1)
    from_high = jnp.concatenate([-sin_t, zeros, tail], axis=1)
    return keep, from_low, from_high


def rotate(t_bf16, keep, from_low, from_high):
    head_dim = t_bf16.shape[1]
    quarter = head_dim // 4
    t_f32 = t_bf16.astype(jnp.float32)
    low = pltpu.roll(t_f32, quarter, 1)
    high = pltpu.roll(t_f32, head_dim - quarter, 1)
    return (t_f32 * keep + low * from_low + high * from_high).astype(jnp.bfloat16)


def strip_attention(q_rot, k_blocks, v_blocks, row0, seq_len):
    head_dim = q_rot[0].shape[1]
    scale = head_dim ** -0.5 * LOG2_E

    def step(diagonal, kb, carry):
        start = pl.multiple_of(kb * KBLK, KBLK)
        k_blk = k_blocks(start)
        v_blk = v_blocks(start)
        length_bias = jnp.where(start + lax.broadcasted_iota(jnp.int32, (1, KBLK), 1) < seq_len, 0.0, -1e30)
        if diagonal:
            rows = row0 + lax.broadcasted_iota(jnp.int32, (QBLK, KBLK), 0)
            cols = start + lax.broadcasted_iota(jnp.int32, (QBLK, KBLK), 1)
            causal = cols <= rows
        out = []
        for q_head, (m_old, l_old, acc) in zip(q_rot, carry):
            s = lax.dot_general(q_head, k_blk, (((1,), (1,)), ((), ())), preferred_element_type=jnp.float32) * scale + length_bias
            if diagonal:
                s = jnp.where(causal, s, -1e30)
            m_new = jnp.maximum(m_old, jnp.max(s, axis=1, keepdims=True))
            corr = jnp.exp2(m_old - m_new)
            p = jnp.exp2(s - m_new)
            l_new = l_old * corr + jnp.sum(p, axis=1, keepdims=True)
            acc = acc * corr + jnp.dot(p.astype(jnp.bfloat16), v_blk, preferred_element_type=jnp.float32)
            out.append((m_new, l_new, acc))
        return tuple(out)

    carry = tuple(
        (jnp.full((QBLK, 1), -1e30, jnp.float32), jnp.zeros((QBLK, 1), jnp.float32), jnp.zeros((QBLK, head_dim), jnp.float32))
        for _ in q_rot
    )
    carry = lax.fori_loop(0, row0 // KBLK, functools.partial(step, False), carry)
    carry = lax.fori_loop(row0 // KBLK, (row0 + QBLK + KBLK - 1) // KBLK, functools.partial(step, True), carry)
    return [(acc / l_sum).astype(jnp.bfloat16) for _, l_sum, acc in carry]


def first_strips_kernel(len_ref, q_ref, k_ref, v_ref, qc_ref, ql_ref, qh_ref, kc_ref, kl_ref, kh_ref, ctx_ref, k_rot_ref):
    head_dim = k_ref.shape[1]

    @pl.when(pl.program_id(1) == 0)
    def _():
        k_rot_ref[...] = rotate(k_ref[...], kc_ref[...], kl_ref[...], kh_ref[...])

    tables = (qc_ref[...], ql_ref[...], qh_ref[...])
    heads = range(0, q_ref.shape[1], head_dim)
    context = strip_attention(
        [rotate(q_ref[:, h:h + head_dim], *tables) for h in heads],
        lambda start: k_rot_ref[pl.ds(start, KBLK), :],
        lambda start: v_ref[pl.ds(start, KBLK), :],
        pl.program_id(1) * (k_ref.shape[0] // 2),
        len_ref[0],
    )
    for h, rows in zip(heads, context):
        ctx_ref[:, h:h + head_dim] = rows


def first_strips(qkv, seq_lens, tables, q_heads, kv_heads, head_dim):
    seq_length = qkv.shape[0]
    width = q_heads // kv_heads * head_dim
    strips = seq_length // 2 // QBLK
    table_q = pl.BlockSpec((QBLK, head_dim), lambda g, i, *_: (i * strips, 0))
    table_k = pl.BlockSpec((seq_length, head_dim), lambda g, i, *_: (0, 0))
    return pl.pallas_call(
        first_strips_kernel,
        grid_spec=pltpu.PrefetchScalarGridSpec(
            num_scalar_prefetch=1,
            grid=(kv_heads, 2),
            in_specs=[
                pl.BlockSpec((QBLK, width), lambda g, i, *_: (i * strips, g)),
                pl.BlockSpec((seq_length, head_dim), lambda g, i, *_: (0, q_heads + g)),
                pl.BlockSpec((seq_length, head_dim), lambda g, i, *_: (0, q_heads + kv_heads + g)),
            ] + [table_q] * 3 + [table_k] * 3,
            out_specs=[
                pl.BlockSpec((QBLK, width), lambda g, i, *_: (i, g)),
                pl.BlockSpec((seq_length, head_dim), lambda g, i, *_: (0, g)),
            ],
        ),
        out_shape=[
            jax.ShapeDtypeStruct((2 * QBLK, q_heads * head_dim), jnp.bfloat16),
            jax.ShapeDtypeStruct((seq_length, kv_heads * head_dim), jnp.bfloat16),
        ],
        compiler_params=pltpu.CompilerParams(dimension_semantics=("arbitrary", "arbitrary"), vmem_limit_bytes=48 << 20),
        cost_estimate=pl.CostEstimate(flops=15 * 10 ** 9, bytes_accessed=12 << 20, transcendentals=0),
        name="first_strips",
    )(seq_lens, qkv, qkv, qkv, *tables, *tables)


class Line:
    def __init__(self, n_tp, half):
        self.z = lax.axis_index("tp")
        self.others = (lax.axis_index("dp"), lax.axis_index("fsdp"))
        self.last = n_tp - 1
        self.place = (self.z, self.last - self.z)
        self.sum_base = (half, 0)
        self.row_base = (0, half)

    def device(self, d):
        return (self.others[0], self.z + (1 if d == 0 else -1), self.others[1])

    def copy(self, d, src, dst, send_sem, recv_sem):
        return pltpu.make_async_remote_copy(
            src_ref=src, dst_ref=dst, send_sem=send_sem, recv_sem=recv_sem,
            device_id=self.device(d), device_id_type=pl.DeviceIdType.MESH,
        )

    def meet(self):
        barrier = pltpu.get_barrier_semaphore()
        for d in range(2):

            @pl.when(self.place[d] < self.last)
            def _():
                pl.semaphore_signal(barrier, inc=1, device_id=self.device(d), device_id_type=pl.DeviceIdType.MESH)

        pl.semaphore_wait(barrier, sum((place < self.last).astype(jnp.int32) for place in self.place))


def own_copies(line, half, pairs):
    for d in range(2):

        @pl.when(line.place[d] == line.last)
        def _():
            pairs(d, line.sum_base[d])


def sum_step(line, d, p, rows, part_ref, sum_ref, send, recv, finish):
    here = pl.ds(pl.multiple_of(p * rows, rows), rows)
    part_rows = pl.ds(pl.multiple_of(line.sum_base[d] + p * rows, rows), rows)
    place = line.place[d]

    @pl.when(place == 0)
    def _():
        line.copy(d, part_ref.at[part_rows], sum_ref.at[d, here], send.at[d, p], recv.at[d, p]).start()

    @pl.when(place > 0)
    def _():
        copy = line.copy(d, sum_ref.at[d, here], sum_ref.at[d, here], send.at[d, p], recv.at[d, p])
        copy.wait_recv()
        total = sum_ref[d, here, :].astype(jnp.float32) + part_ref[part_rows, :].astype(jnp.float32)

        @pl.when(place < line.last)
        def _():
            sum_ref[d, here, :] = total.astype(jnp.bfloat16)
            copy.start()

        @pl.when(place == line.last)
        def _():
            rows_done = (sum_ref[1 - d, here, :].astype(jnp.float32) + total).astype(jnp.bfloat16)
            sum_ref[d, here, :] = rows_done
            finish(here, part_rows, rows_done)


def drain_sums(line, rows, part_ref, sum_ref, send, recv, finished):
    def body(p, _):
        here = pl.ds(pl.multiple_of(p * rows, rows), rows)
        for d in range(2):

            @pl.when(line.place[d] < line.last)
            def _():
                line.copy(d, sum_ref.at[d, here], sum_ref.at[d, here], send.at[d, p], recv.at[d, p]).wait_send()

            @pl.when(line.place[d] == line.last)
            def _():
                finished(d, p, here)

        return 0

    lax.fori_loop(0, PIECES, body, 0)


def attend_reduce_kernel(n_tp, q_heads, len_ref, qkv, k_rot, keep, from_low, from_high, gain_ref, first_hbm, o_hbm, x_hbm,
                         x_own_hbm, h_own_hbm, o_full, part, sums, ctx, load_sem, x_sem, send, recv, x_out, h_out):
    half = part.shape[0] // 2
    rows = half // PIECES
    strips = half // QBLK
    per_strip = PIECES // strips
    head_dim = keep.shape[1]
    kv_heads = k_rot.shape[1] // head_dim
    group = q_heads // kv_heads
    line = Line(n_tp, half)
    loads = (pltpu.make_async_copy(first_hbm, ctx, load_sem.at[0]), pltpu.make_async_copy(o_hbm, o_full, load_sem.at[1]))
    for load in loads:
        load.start()

    def own(d, row):
        return pltpu.make_async_copy(x_hbm.at[pl.ds(row, half)], sums.at[1 - d], x_sem)

    own_copies(line, half, lambda d, row: own(d, row).start())
    line.meet()
    for load in loads:
        load.wait()
    seq_len = len_ref[0]

    def lanes_of(index, size):
        return pl.ds(pl.multiple_of(index * size, size), size)

    def output_product(strip):
        def tile(n, _):
            lanes = lanes_of(n, TILE)
            for k in range(2):
                product = jnp.dot(ctx[k * QBLK:(k + 1) * QBLK, :], o_full[:, lanes], preferred_element_type=jnp.float32)
                part[pl.ds(pl.multiple_of(k * half + strip * QBLK, QBLK), QBLK), lanes] = product.astype(jnp.bfloat16)
            return 0

        lax.fori_loop(0, part.shape[1] // TILE, tile, 0)

    def attend(strip, k, kv, heads):
        row0 = pl.multiple_of(k * half + strip * QBLK, QBLK)
        q_rows = pl.ds(row0, QBLK)
        tables = (keep[q_rows, :], from_low[q_rows, :], from_high[q_rows, :])
        context = strip_attention(
            [rotate(qkv[q_rows, lanes_of(kv * group + h, head_dim)], *tables) for h in heads],
            lambda start: k_rot[pl.ds(start, KBLK), lanes_of(kv, head_dim)],
            lambda start: qkv[pl.ds(start, KBLK), lanes_of(q_heads + kv_heads + kv, head_dim)],
            row0,
            seq_len,
        )
        for h, context_rows in zip(heads, context):
            ctx[pl.ds(pl.multiple_of(k * QBLK, QBLK), QBLK), lanes_of(kv * group + h, head_dim)] = context_rows

    output_product(0)
    own_copies(line, half, lambda d, row: own(d, row).wait())

    def outward(d, p, here):
        part_rows = pl.ds(pl.multiple_of(line.sum_base[d] + p * rows, rows), rows)
        return (
            pltpu.make_async_copy(sums.at[d, here], x_own_hbm.at[here], x_out.at[p]),
            pltpu.make_async_copy(part.at[part_rows], h_own_hbm.at[here], h_out.at[p]),
        )

    def step(t, _):
        for d in range(2):
            p = t - line.place[d]

            def finish(here, part_rows, rows_done, d=d, p=p):
                part[part_rows, :] = layer_norm(rows_done, gain_ref[...])
                for copy in outward(d, p, here):
                    copy.start()

            @pl.when((p >= 0) & (p < PIECES))
            def _():
                sum_step(line, d, p, rows, part, sums, send, recv, finish)

            strip = t // per_strip + 1
            unit = t % per_strip

            @pl.when((strip < strips) & (unit < 2 * kv_heads))
            def _():
                heads = range(group // 2 * d, group // 2 + (group - group // 2) * d)
                attend(strip, unit // kv_heads, unit % kv_heads, heads)

        @pl.when((strip < strips) & (unit == per_strip - 1))
        def _():
            output_product(strip)

        return 0

    lax.fori_loop(0, PIECES + line.last, step, 0)

    def finished(d, p, here):
        for copy in outward(d, p, here):
            copy.wait()

    drain_sums(line, rows, part, sums, send, recv, finished)


def mlp_kernel(n_tp, x_own_hbm, h_own_hbm, up_hbm, down_hbm, out_hbm, up, down, h, sums, act,
               w_sem, own_sem, h_send, h_recv, send, recv, y_send, y_recv, y_out):
    half = h.shape[0] // 2
    rows = half // PIECES
    group_rows = rows * PER_GROUP
    groups = PIECES // PER_GROUP
    up_tiles, down_tiles = up.shape[1] // TILE, down.shape[1] // TILE
    per_step = pl.cdiv(up_tiles + down_tiles, PER_GROUP)
    line = Line(n_tp, half)
    first = PER_GROUP + line.last
    loads = (pltpu.make_async_copy(up_hbm, up, w_sem.at[0]), pltpu.make_async_copy(down_hbm, down, w_sem.at[1]))

    def own(d, row):
        return (
            pltpu.make_async_copy(x_own_hbm, sums.at[1 - d], own_sem.at[0]),
            pltpu.make_async_copy(h_own_hbm, h.at[pl.ds(row, half)], own_sem.at[1]),
        )

    own_copies(line, half, lambda d, row: [c.start() for c in reversed(own(d, row))])
    for load in loads:
        load.start()
    line.meet()
    own_copies(line, half, lambda d, row: own(d, row)[1].wait())

    def row_slice(d, p):
        return pl.ds(pl.multiple_of(line.row_base[d] + p * rows, rows), rows)

    def h_copy(d, p):
        return line.copy(d, h.at[row_slice(d, p)], h.at[row_slice(d, p)], h_send.at[d, p], h_recv.at[d, p])

    def y_local(d, p, here):
        return pltpu.make_async_copy(sums.at[d, here], out_hbm.at[row_slice(1 - d, p)], y_out.at[p])

    def y_first(d, p):
        here = pl.ds(pl.multiple_of(p * rows, rows), rows)
        return line.copy(d, sums.at[1 - d, here], out_hbm.at[row_slice(d, p)], y_send.at[d, p], y_recv.at[d, p])

    def y_next(d, p):
        return line.copy(d, out_hbm.at[row_slice(d, p)], out_hbm.at[row_slice(d, p)], y_send.at[d, p], y_recv.at[d, p])

    def group_slices(g):
        return [pl.ds(pl.multiple_of(base + g * group_rows, group_rows), group_rows) for base in (0, half)]

    def product(g, unit):
        @pl.when(unit < up_tiles)
        def _():
            lanes = pl.ds(pl.multiple_of(unit * TILE, TILE), TILE)
            for k, group in enumerate(group_slices(g)):
                pre = jnp.dot(h[group, :], up[:, lanes], preferred_element_type=jnp.float32)
                act[k * group_rows:(k + 1) * group_rows, lanes] = jnp.square(jnp.maximum(pre, 0.0)).astype(jnp.bfloat16)

        @pl.when(unit == up_tiles)
        def _():
            for q in range(PER_GROUP):
                for d in range(2):

                    @pl.when(line.place[d] < line.last)
                    def _():
                        h_copy(d, g * PER_GROUP + q).wait_send()

        @pl.when((unit >= up_tiles) & (unit < up_tiles + down_tiles))
        def _():
            lanes = pl.ds(pl.multiple_of((unit - up_tiles) * TILE, TILE), TILE)
            for k, group in enumerate(group_slices(g)):
                part = jnp.dot(act[k * group_rows:(k + 1) * group_rows, :], down[:, lanes], preferred_element_type=jnp.float32)
                h[group, lanes] = part.astype(jnp.bfloat16)

    def step(t, _):
        for d in range(2):
            place = line.place[d]
            m = t - place

            @pl.when((m >= 0) & (m < PIECES))
            def _():
                @pl.when(place > 0)
                def _():
                    h_copy(d, m).wait_recv()

                @pl.when(place < line.last)
                def _():
                    h_copy(d, m).start()

            p = m - PIECES

            def finish(here, part_rows, rows_done, d=d, p=p):
                y_local(d, p, here).start()

            @pl.when((p >= 0) & (p < PIECES))
            def _():
                sum_step(line, d, p, rows, h, sums, send, recv, finish)

            q = m - 2 * PIECES

            @pl.when((q >= 0) & (q < PIECES))
            def _():
                @pl.when(place == 0)
                def _():
                    y_first(d, q).start()

                @pl.when(place > 0)
                def _():
                    y_next(d, q).wait_recv()

                    @pl.when(place < line.last)
                    def _():
                        y_next(d, q).start()

        @pl.when(t == first)
        def _():
            own_copies(line, half, lambda d, row: own(d, row)[0].wait())
            for load in loads:
                load.wait()

        k = t - first

        @pl.when((k >= 0) & (k < PIECES))
        def _():
            def units(u, _):
                product(k // PER_GROUP, (k % PER_GROUP) * per_step + u)
                return 0

            lax.fori_loop(0, per_step, units, 0)

        return 0

    lax.fori_loop(0, 3 * PIECES + line.last, step, 0)
    drain_sums(line, rows, h, sums, send, recv, lambda d, p, here: y_local(d, p, here).wait())

    def drain(p, _):
        for d in range(2):

            @pl.when(line.place[d] < line.last)
            def _():
                y_next(d, p).wait_send()

        return 0

    lax.fori_loop(0, PIECES, drain, 0)


def attend_reduce(n_tp, q_heads, seq_lens, qkv, k_rot, tables, gain, first_ctx, o_full, x_rows):
    seq_length, width = x_rows.shape
    half = seq_length // 2
    own = jax.ShapeDtypeStruct((half, width), jnp.bfloat16)
    any_spec = pl.BlockSpec(memory_space=pl.ANY)
    vmem_spec = pl.BlockSpec(memory_space=pltpu.VMEM)
    dma = pltpu.SemaphoreType.DMA
    return pl.pallas_call(
        functools.partial(attend_reduce_kernel, n_tp, q_heads),
        in_specs=[pl.BlockSpec(memory_space=pltpu.SMEM)] + [vmem_spec] * 6 + [any_spec] * 3,
        out_specs=[any_spec, any_spec],
        out_shape=[own, own],
        scratch_shapes=[
            pltpu.VMEM(o_full.shape, jnp.bfloat16),
            pltpu.VMEM((seq_length, width), jnp.bfloat16),
            pltpu.VMEM((2, half, width), jnp.bfloat16),
            pltpu.VMEM(first_ctx.shape, jnp.bfloat16),
            dma((2,)), dma, dma((2, PIECES)), dma((2, PIECES)), dma((PIECES,)), dma((PIECES,)),
        ],
        compiler_params=pltpu.CompilerParams(collective_id=0, has_side_effects=True, vmem_limit_bytes=60 << 20),
        cost_estimate=pl.CostEstimate(flops=150 * 10 ** 9, bytes_accessed=32 << 20, transcendentals=0),
        name="attend_reduce",
    )(seq_lens, qkv, k_rot, *tables, gain.reshape(1, width), first_ctx, o_full, x_rows)


def mlp_rows(n_tp, x_own, h_own, up_full, down_full):
    half, width = x_own.shape
    hidden = up_full.shape[1]
    any_spec = pl.BlockSpec(memory_space=pl.ANY)
    dma = pltpu.SemaphoreType.DMA
    return pl.pallas_call(
        functools.partial(mlp_kernel, n_tp),
        in_specs=[any_spec] * 4,
        out_specs=any_spec,
        out_shape=jax.ShapeDtypeStruct((2 * half, width), jnp.bfloat16),
        scratch_shapes=[
            pltpu.VMEM((width, hidden), jnp.bfloat16),
            pltpu.VMEM((hidden, width), jnp.bfloat16),
            pltpu.VMEM((2 * half, width), jnp.bfloat16),
            pltpu.VMEM((2, half, width), jnp.bfloat16),
            pltpu.VMEM((2 * half // PIECES * PER_GROUP, hidden), jnp.bfloat16),
            dma((2,)), dma((2,)),
        ] + [dma((2, PIECES))] * 6 + [dma((PIECES,))],
        compiler_params=pltpu.CompilerParams(collective_id=1, has_side_effects=True, vmem_limit_bytes=63 << 20),
        cost_estimate=pl.CostEstimate(flops=400 * 10 ** 9, bytes_accessed=64 << 20, transcendentals=0),
        name="mlp_rows",
    )(x_own, h_own, up_full, down_full)


def solution(mesh):
    batch_axes = ("dp", "fsdp")
    arg_specs = (P(batch_axes, None, None), P(batch_axes), P(None), P("fsdp", "tp", None), P("fsdp", "tp", None), P("fsdp", "tp", None), P("tp", None, "fsdp"), P(None), P("fsdp", "tp"), P("tp", "fsdp"))
    out_parts = (P(batch_axes, None, None), P(batch_axes, None, "tp", None), P(batch_axes, None, "tp", None))
    n_tp = mesh.shape["tp"]

    def layer_local(x_in, seq_lens, ln1_gain, w_q, w_k, w_v, w_o, ln2_gain, w_up, w_down):
        _, seq_length, width = x_in.shape
        q_heads, kv_heads, head_dim = w_q.shape[1], w_k.shape[1], w_k.shape[2]
        x_rows = x_in.reshape(seq_length, width)

        w_qkv = jnp.concatenate([w.reshape(w.shape[0], -1) for w in (w_q, w_k, w_v)], axis=1)
        qkv_full = lax.all_gather(w_qkv, "fsdp", axis=0, tiled=True)
        o_full = lax.all_gather(w_o.reshape(q_heads * head_dim, -1), "fsdp", axis=1, tiled=True)
        up_full = lax.all_gather(w_up, "fsdp", axis=0, tiled=True)
        down_full = lax.all_gather(w_down, "fsdp", axis=1, tiled=True)

        tables = rotary_tables(seq_length, head_dim)
        h_norm = layer_norm(x_rows, ln1_gain)
        qkv = jnp.dot(h_norm, qkv_full, preferred_element_type=jnp.float32).astype(jnp.bfloat16)
        first_ctx, k_rot = first_strips(qkv, seq_lens, tables, q_heads, kv_heads, head_dim)
        v_loc = qkv[:, (q_heads + kv_heads) * head_dim:]
        x_own, h_own = attend_reduce(n_tp, q_heads, seq_lens, qkv, k_rot, tables, ln2_gain, first_ctx, o_full, x_rows)
        out = mlp_rows(n_tp, x_own, h_own, up_full, down_full)

        y_out = out.reshape(1, seq_length, width)
        k_cache = k_rot.reshape(1, seq_length, kv_heads, head_dim)
        v_cache = v_loc.reshape(1, seq_length, kv_heads, head_dim)
        return y_out, k_cache, v_cache

    return jax.shard_map(layer_local, mesh=mesh, in_specs=arg_specs, out_specs=out_parts, check_vma=False)
```
